32 devices in a mesh: seq: 8 (over y, x, core), dp: 4 (over z).
Axes of the slice: x: 2, y: 2, z: 4, core: 2. Of those that a mesh axis runs over, the one named last changes fastest.
Arguments:
- queries: bfloat16 [4, 3072, 2048], P('dp', 'seq'), may hold values from -40 to 40
- keys: bfloat16 [4, 3072, 2048], P('dp', 'seq'), may hold values from -40 to 40
- values: bfloat16 [4, 3072, 2048], P('dp', 'seq'), may hold values from -6 to 6
- out_grad: bfloat16 [4, 3072, 2048], P('dp', 'seq'), may hold values from -6 to 6
- proj_weight: bfloat16 [2048, 2048], P('dp'), may hold values from -0.125 to 0.125
- lengths: int32 [4], P('dp'), may hold values from 768 to 3072
Outputs:
- query_grad: bfloat16 [4, 3072, 2048], P('dp', 'seq')
- key_grad: bfloat16 [4, 3072, 2048], P('dp', 'seq')
- value_grad: bfloat16 [4, 3072, 2048], P('dp', 'seq')
- weight_grad: float32 [2048, 2048], P('dp', 'seq')
The draws below stay inside these ranges and needn't reach their ends.
All inputs are finite; a program needn't handle non-finite values.
Results may differ from the reference program's by a relative error of at most 0.019.
Values may be sent and summed in bfloat16 or wider, within the bound.
A program may use at most 192 MiB of HBM per device.

```python
import jax
import jax.numpy as jnp
from jax import lax

HEADS = 16
HEAD_DIM = 128
DW = 2048
CYCLE = 2
TOK_DEV = 384
FEAT = 2048
TOKENS = 3072
SEQS = 4
N_SEQ = 8


def paired_rows(key):
    base = jax.random.fold_in(key, 7)
    query_draw = jax.random.normal(jax.random.fold_in(base, 1), (SEQS, TOKENS, FEAT), jnp.float32)
    key_draw = jax.random.normal(jax.random.fold_in(base, 2), (SEQS, TOKENS, FEAT), jnp.float32)
    query_draw = jnp.clip(query_draw, -40.0, 40.0)
    key_draw = jnp.clip(key_draw, -40.0, 40.0)
    return (query_draw, key_draw)


def draw_queries(key, part):
    return paired_rows(key)[0].astype(jnp.bfloat16)


def draw_keys(key, part):
    return paired_rows(key)[1].astype(jnp.bfloat16)


def with_ends(values, stream_key, smallest, largest):
    index_at = [jax.random.randint(jax.random.fold_in(stream_key, axis), (), 0, length) for axis, length in enumerate(values.shape)]
    longest = values.shape.index(max(values.shape))
    next_to = index_at[:longest] + [(index_at[longest] + 1) % values.shape[longest]] + index_at[longest + 1:]
    return values.at[tuple(index_at)].set(smallest).at[tuple(next_to)].set(largest)


def strengthened(values, own_key, source, target, shards_of, factor):
    owner, partner = [(jnp.arange(values.shape[dim]) // (values.shape[dim] // shards_of)).reshape([-1 if axis == dim else 1 for axis in range(values.ndim)]) for dim in (source, target)]
    chosen = jax.random.permutation(own_key, shards_of)[partner]
    strong = (owner == chosen) | (owner == (partner + shards_of // 2) % shards_of)
    return jnp.where(strong, factor * values, values)


def level_of(key, extent, pieces, smallest, high):
    gain = 1.0
    for dim, blocks in pieces:
        draws = jax.random.uniform(jax.random.fold_in(jax.random.fold_in(key, 6), dim), (blocks,), jnp.float32, smallest / len(pieces), high / len(pieces))
        gain = gain * jnp.repeat(jnp.exp(draws), extent[dim] // blocks).reshape((-1,) + (1,) * (len(extent) - 1 - dim))
    return gain


def bell_draw(stream_key, dims, spread, most, cuts=(), held_as=jnp.bfloat16):
    drawn = spread * jax.random.normal(stream_key, dims, jnp.float32)
    if cuts:
        drawn = drawn * level_of(stream_key, dims, cuts, -0.22, 0.18)
    return jnp.clip(drawn, -most, most).astype(held_as)


def heavy_noise(rng, shape, deviation, bound, shards, heavy, held_as=jnp.bfloat16):
    drawn = deviation * jax.random.normal(rng, shape, jnp.float32)
    if shards:
        drawn = drawn * level_of(rng, shape, shards, -0.22, 0.18)
    return jnp.clip(strengthened(drawn, jax.random.fold_in(rng, 3), *heavy), -bound, bound).astype(held_as)


def setup_inputs(seed: int = 0) -> dict:
    arg_keys = jax.random.split(jax.random.key(seed), 7)
    return {
        "queries": draw_queries(jax.random.fold_in(arg_keys[6], 71), 0),
        "keys": draw_keys(jax.random.fold_in(arg_keys[6], 71), 0),
        "values": bell_draw(arg_keys[2], (SEQS, TOKENS, FEAT), 1.0, 6.0, ((0, 4), (1, 8))),
        "out_grad": heavy_noise(arg_keys[3], (SEQS, TOKENS, DW), 1.0, 6.0, ((0, 4), (1, 8)), (1, 2, 8, 2.0)),
        "proj_weight": bell_draw(arg_keys[4], (FEAT, DW), FEAT ** -0.5, 0.125, ((0, 4),)),
        "lengths": with_ends(jax.random.randint(arg_keys[5], (SEQS,), TOKENS // 4, TOKENS + 1), jax.random.fold_in(arg_keys[5], 1), TOKENS // 4, TOKENS).astype(jnp.int32),
    }


def reference(queries, keys, values, out_grad, proj_weight, lengths):
    scale = HEAD_DIM ** -0.5
    window = (CYCLE + 1) * TOK_DEV
    leading = CYCLE * TOK_DEV
    weight_total = jnp.zeros((FEAT, DW), jnp.float32)
    query_list = []
    key_list = []
    value_list = []
    for batch in range(SEQS):
        query_seq = queries[batch]
        grad_seq = out_grad[batch]
        front = jnp.zeros((leading, FEAT), jnp.bfloat16)
        key_padded = jnp.concatenate([front, keys[batch]], 0)
        value_padded = jnp.concatenate([front, values[batch]], 0)
        limit = lengths[batch]

        def block_step(carry, index):
            key_accum, value_accum, weight_accum = carry
            first = (index * TOK_DEV).astype(jnp.int32)
            query_block = lax.dynamic_slice_in_dim(query_seq, first, TOK_DEV, 0)
            grad_block = lax.dynamic_slice_in_dim(grad_seq, first, TOK_DEV, 0)
            key_window = lax.dynamic_slice_in_dim(key_padded, first, window, 0)
            value_window = lax.dynamic_slice_in_dim(value_padded, first, window, 0)
            query_pos = first + jnp.arange(TOK_DEV, dtype=jnp.int32)
            key_pos = first - leading + jnp.arange(window, dtype=jnp.int32)
            allowed = (key_pos[None, :] >= 0) & (key_pos[None, :] <= query_pos[:, None])
            query_heads = query_block.reshape(TOK_DEV, HEADS, HEAD_DIM).astype(jnp.float32)
            key_heads = key_window.reshape(window, HEADS, HEAD_DIM).astype(jnp.float32)
            value_heads = value_window.reshape(window, HEADS, HEAD_DIM).astype(jnp.float32)
            scores = jnp.einsum("thd,shd->hts", query_heads, key_heads) * scale
            scores = jnp.where(allowed[None], scores, -1e30)
            maximum = jnp.max(scores, axis=2, keepdims=True)
            lse = maximum + jnp.log(jnp.sum(jnp.exp(scores - maximum), axis=2, keepdims=True))
            probs = jnp.exp(scores - lse)
            probs_b = probs.astype(jnp.bfloat16)
            attn_out = jnp.einsum("hts,shd->thd", probs_b.astype(jnp.float32), value_heads).astype(jnp.bfloat16)
            live = (query_pos < limit).astype(jnp.bfloat16)
            grad_masked = grad_block * live[:, None]
            out_bwd = jnp.dot(grad_masked, proj_weight.T, preferred_element_type=jnp.float32).astype(jnp.bfloat16)
            attn_flat = attn_out.reshape(TOK_DEV, FEAT)
            weight_accum = weight_accum + lax.dot_general(attn_flat, grad_masked, (((0,), (0,)), ((), ())), preferred_element_type=jnp.float32)
            out_heads = out_bwd.reshape(TOK_DEV, HEADS, HEAD_DIM).astype(jnp.float32)
            delta = jnp.sum(out_heads * attn_out.astype(jnp.float32), axis=2)
            prob_grad = jnp.einsum("thd,shd->hts", out_heads, value_heads)
            score_grad = (probs * (prob_grad - delta.T[:, :, None]) * scale).astype(jnp.bfloat16)
            score_f = score_grad.astype(jnp.float32)
            query_grad = jnp.einsum("hts,shd->thd", score_f, key_heads).astype(jnp.bfloat16)
            key_term = jnp.einsum("hts,thd->shd", score_f, query_heads).astype(jnp.bfloat16)
            value_term = jnp.einsum("hts,thd->shd", probs_b.astype(jnp.float32), out_heads).astype(jnp.bfloat16)
            key_old = lax.dynamic_slice_in_dim(key_accum, first, window, 0)
            value_old = lax.dynamic_slice_in_dim(value_accum, first, window, 0)
            key_accum = lax.dynamic_update_slice_in_dim(key_accum, key_old + key_term.reshape(window, FEAT).astype(jnp.float32), first, 0)
            value_accum = lax.dynamic_update_slice_in_dim(value_accum, value_old + value_term.reshape(window, FEAT).astype(jnp.float32), first, 0)
            return (key_accum, value_accum, weight_accum), query_grad.reshape(TOK_DEV, FEAT)

        start_carry = (jnp.zeros((TOKENS + leading, FEAT), jnp.float32), jnp.zeros((TOKENS + leading, FEAT), jnp.float32), weight_total)
        final_carry, query_blocks = lax.scan(block_step, start_carry, jnp.arange(N_SEQ, dtype=jnp.int32))
        key_accum, value_accum, weight_total = final_carry
        query_list.append(query_blocks.reshape(TOKENS, FEAT))
        key_list.append(key_accum[leading:].astype(jnp.bfloat16))
        value_list.append(value_accum[leading:].astype(jnp.bfloat16))
    return (jnp.stack(query_list), jnp.stack(key_list), jnp.stack(value_list), weight_total)
```

```python
import functools

import jax
import jax.numpy as jnp
from jax import lax
from jax.experimental import pallas as pl
from jax.experimental.pallas import tpu as pltpu
from jax.sharding import PartitionSpec as P

HEAD_DIM = 128
CYCLE = 2
GROUPS = 2
LOG2E = 1.4426950408889634
NEG = -1e30

NT = (((1,), (1,)), ((), ()))
NN = (((1,), (0,)), ((), ()))
TN = (((0,), (0,)), ((), ()))


def dot(a, b, dims):
    return lax.dot_general(a, b, dims, preferred_element_type=jnp.float32)


def scores_t(k, q, causal):
    s = dot(k, q, NT)
    if causal:
        key_at = lax.broadcasted_iota(jnp.int32, s.shape, 0)
        query_at = lax.broadcasted_iota(jnp.int32, s.shape, 1)
        s = jnp.where(key_at <= query_at, s, NEG)
    return s


def fwd_kernel(pos, q_ref, k0, k1, k2, v0, v1, v2, o_ref, lse_ref):
    c = HEAD_DIM ** (-0.5) * LOG2E
    q = q_ref[...]
    parts = []
    for offset, k in enumerate((k0, k1, k2)):
        parts.append(scores_t(k[...], q, offset == 0))
    tops = [jnp.max(parts[0], axis=0, keepdims=True)]
    for offset in (1, 2):
        off = jnp.where(pos[0] >= offset, 0.0, NEG)
        tops.append(jnp.max(parts[offset], axis=0, keepdims=True) + off)
    top = functools.reduce(jnp.maximum, tops) * c
    total = None
    out = None
    for offset, v in enumerate((v0, v1, v2)):
        off = jnp.where(pos[0] >= offset, 0.0, -NEG)
        e = jnp.exp2(parts[offset] * c - (top + off))
        t = jnp.sum(e, axis=0, keepdims=True)
        o = dot(v[...], e.astype(jnp.bfloat16), TN)
        total = t if total is None else total + t
        out = o if out is None else out + o
    out = out * (1.0 / total)
    o_ref[...] = out.T.astype(jnp.bfloat16)
    lse_ref[0] = top + jnp.log2(total)


def bwd_kernel(
    pos, q_ref, k0, k1, k2, v0, v1, v2, o_ref, lse_ref, do_ref,
    dq_ref, dk0, dk1, dk2, dv0, dv1, dv2,
):
    scale = HEAD_DIM ** (-0.5)
    c = scale * LOG2E
    q = q_ref[...]
    do = do_ref[...]
    prod = do.astype(jnp.float32) * o_ref[...].astype(jnp.float32)
    delta = jnp.sum(prod.T, axis=0, keepdims=True)
    lse = lse_ref[0]
    dq = None
    for offset, (k_ref, v_ref, dk, dv) in enumerate(
        ((k0, v0, dk0, dv0), (k1, v1, dk1, dv1), (k2, v2, dk2, dv2))
    ):
        k = k_ref[...]
        off = jnp.where(pos[0] >= offset, 0.0, -NEG)
        s = scores_t(k, q, offset == 0)
        p = jnp.exp2(s * c - (lse + off))
        dv[...] = dot(p.astype(jnp.bfloat16), do, NN).astype(jnp.bfloat16)
        dp = dot(v_ref[...], do, NT)
        ds = (p * (dp - delta)).astype(jnp.bfloat16)
        dk[...] = (dot(ds, q, NN) * scale).astype(jnp.bfloat16)
        part = dot(k, ds, TN)
        dq = part if dq is None else dq + part
    dq_ref[...] = (dq * scale).T.astype(jnp.bfloat16)


def head_specs(tokens, count):
    return [pl.BlockSpec((tokens, HEAD_DIM), lambda h, pos: (0, h))] * count


def lse_spec(tokens):
    return pl.BlockSpec((1, 1, tokens), lambda h, pos: (h, 0, 0))


def forward(pos, q, ks, vs):
    tokens, width = q.shape
    heads = width // HEAD_DIM
    pairs = heads * tokens * tokens * 3
    return pl.pallas_call(
        fwd_kernel,
        grid_spec=pltpu.PrefetchScalarGridSpec(
            num_scalar_prefetch=1,
            grid=(heads,),
            in_specs=head_specs(tokens, 7),
            out_specs=head_specs(tokens, 1) + [lse_spec(tokens)],
        ),
        out_shape=[
            jax.ShapeDtypeStruct((tokens, width), jnp.bfloat16),
            jax.ShapeDtypeStruct((heads, 1, tokens), jnp.float32),
        ],
        cost_estimate=pl.CostEstimate(
            flops=pairs * HEAD_DIM * 12, bytes_accessed=tokens * width * 16, transcendentals=pairs
        ),
        name="attn_fwd",
    )(pos, q, *ks, *vs)


def backward(pos, q, ks, vs, o, lse, do):
    tokens, width = q.shape
    heads = width // HEAD_DIM
    pairs = heads * tokens * tokens * 3
    return pl.pallas_call(
        bwd_kernel,
        grid_spec=pltpu.PrefetchScalarGridSpec(
            num_scalar_prefetch=1,
            grid=(heads,),
            in_specs=head_specs(tokens, 8) + [lse_spec(tokens)] + head_specs(tokens, 1),
            out_specs=head_specs(tokens, 7),
        ),
        out_shape=[jax.ShapeDtypeStruct((tokens, width), jnp.bfloat16)] * 7,
        cost_estimate=pl.CostEstimate(
            flops=pairs * HEAD_DIM * 24, bytes_accessed=tokens * width * 32, transcendentals=pairs
        ),
        name="attn_bwd",
    )(pos, q, *ks, *vs, o, lse, do)


def shifted(block, distance):
    devices = range(lax.axis_size("seq"))
    route = [(i - distance, i) for i in devices if i - distance in devices]
    return lax.ppermute(block, "seq", route)


def swapped(block):
    route = [(i, i ^ 1) for i in range(lax.axis_size("seq"))]
    return lax.ppermute(block, "seq", route)


def per_device(queries, keys, values, out_grad, proj_weight, lengths):
    f32, bf16 = jnp.float32, jnp.bfloat16
    tokens, width = queries.shape[1:]
    place = lax.axis_index("seq")
    odd = lax.rem(place, 2) == 1
    pos = place.astype(jnp.int32).reshape(1)
    query_pos = place * tokens + jnp.arange(tokens, dtype=jnp.int32)
    live = (query_pos < lengths[0]).astype(bf16)
    grad_masked = out_grad[0] * live[:, None]

    part = width // GROUPS
    groups = [slice(g * part, (g + 1) * part) for g in range(GROUPS)]
    held = []
    for g in groups:
        k0, v0 = keys[0][:, g], values[0][:, g]
        k2, v2 = shifted(k0, 2), shifted(v0, 2)
        k1 = swapped(jnp.where(odd, k2, k0))
        v1 = swapped(jnp.where(odd, v2, v0))
        held.append((queries[0][:, g], (k0, k1, k2), (v0, v1, v2)))

    half = proj_weight.shape[1] // 2
    mine = lax.rem(place, 2) * half
    w_mine = lax.all_gather(
        lax.dynamic_slice_in_dim(proj_weight, mine, half, 1), "dp", axis=0, tiled=True
    )
    w_other = swapped(w_mine)

    outs = []
    for q, ks, vs in held:
        outs.append(forward(pos, q, ks, vs))

    attn = jnp.concatenate([o for o, _ in outs], 1)
    term = dot(attn, grad_masked, TN).astype(bf16)
    column_sums = lax.psum_scatter(term, "seq", scatter_dimension=1, tiled=True)
    weight_grad = lax.psum_scatter(
        column_sums.astype(f32), "dp", scatter_dimension=0, tiled=True
    )

    grad_mine = lax.dynamic_slice_in_dim(grad_masked, mine, half, 1)
    grad_other = lax.dynamic_slice_in_dim(grad_masked, half - mine, half, 1)
    out_bwd = (dot(grad_mine, w_mine, NT) + dot(grad_other, w_other, NT)).astype(bf16)

    dqs, dks, dvs = [], [], []
    for g, (q, ks, vs), (o, lse) in zip(groups, held, outs):
        dq, dk0, dk1, dk2, dv0, dv1, dv2 = backward(pos, q, ks, vs, o, lse, out_bwd[:, g])
        dqs.append(dq)
        for into, t0, t1, t2 in ((dks, dk0, dk1, dk2), (dvs, dv0, dv1, dv2)):
            near = swapped(t1).astype(f32)
            zero = jnp.zeros_like(near)
            far = (t2.astype(f32) + jnp.where(odd, near, zero)).astype(bf16)
            far = shifted(far, -2).astype(f32)
            into.append((t0.astype(f32) + jnp.where(odd, zero, near) + far).astype(bf16))
    return (
        jnp.concatenate(dqs, 1)[None],
        jnp.concatenate(dks, 1)[None],
        jnp.concatenate(dvs, 1)[None],
        weight_grad,
    )


def solution(mesh):
    rows = P("dp", "seq", None)
    return jax.shard_map(
        per_device,
        mesh=mesh,
        in_specs=(rows, rows, rows, rows, P("dp", None), P("dp")),
        out_specs=(rows, rows, rows, P("dp", "seq")),
        check_vma=False,
    )
```

```python
import functools

import jax
import jax.numpy as jnp
from jax import lax
from jax.experimental import pallas as pl
from jax.experimental.pallas import tpu as pltpu
from jax.sharding import PartitionSpec as P


HEAD_DIM = 128
GROUPS = 2
LOG2E = 1.4426950408889634
NEG = -1e30

NT = (((1,), (1,)), ((), ()))
NN = (((1,), (0,)), ((), ()))
TN = (((0,), (0,)), ((), ()))


def dot(a, b, dims):
    return lax.dot_general(a, b, dims, preferred_element_type=jnp.float32)


def scores_t(k, q, causal):
    s = dot(k, q, NT)
    if causal:
        key_at = lax.broadcasted_iota(jnp.int32, s.shape, 0)
        query_at = lax.broadcasted_iota(jnp.int32, s.shape, 1)
        s = jnp.where(key_at <= query_at, s, NEG)
    return s


def fwd_kernel(pos, q_ref, k0, k1, k2, v0, v1, v2, o_ref, lse_ref):
    c = HEAD_DIM ** (-0.5) * LOG2E
    q = q_ref[...]
    parts = []
    for offset, k in enumerate((k0, k1, k2)):
        parts.append(scores_t(k[...], q, offset == 0))
    tops = [jnp.max(parts[0], axis=0, keepdims=True)]
    for offset in (1, 2):
        off = jnp.where(pos[0] >= offset, 0.0, NEG)
        tops.append(jnp.max(parts[offset], axis=0, keepdims=True) + off)
    top = functools.reduce(jnp.maximum, tops) * c
    total = None
    out = None
    for offset, v in enumerate((v0, v1, v2)):
        off = jnp.where(pos[0] >= offset, 0.0, -NEG)
        e = jnp.exp2(parts[offset] * c - (top + off))
        t = jnp.sum(e, axis=0, keepdims=True)
        o = dot(v[...], e.astype(jnp.bfloat16), TN)
        total = t if total is None else total + t
        out = o if out is None else out + o
    out = out * (1.0 / total)
    o_ref[...] = out.T.astype(jnp.bfloat16)
    lse_ref[0] = top + jnp.log2(total)


def bwd_kernel(
    pos, q_ref, k0, k1, k2, v0, v1, v2, o_ref, lse_ref, do_ref,
    dq_ref, t0, t1, t2,
):
    scale = HEAD_DIM ** (-0.5)
    c = scale * LOG2E
    q = q_ref[...]
    do = do_ref[...]
    prod = do.astype(jnp.float32) * o_ref[...].astype(jnp.float32)
    delta = jnp.sum(prod.T, axis=0, keepdims=True)
    lse = lse_ref[0]
    dq = None
    for offset, (k_ref, v_ref, term) in enumerate(((k0, v0, t0), (k1, v1, t1), (k2, v2, t2))):
        k = k_ref[...]
        off = jnp.where(pos[0] >= offset, 0.0, -NEG)
        s = scores_t(k, q, offset == 0)
        p = jnp.exp2(s * c - (lse + off))
        term[1] = dot(p.astype(jnp.bfloat16), do, NN).astype(jnp.bfloat16)
        dp = dot(v_ref[...], do, NT)
        ds = (p * (dp - delta)).astype(jnp.bfloat16)
        term[0] = (dot(ds, q, NN) * scale).astype(jnp.bfloat16)
        part = dot(k, ds, TN)
        dq = part if dq is None else dq + part
    dq_ref[...] = (dq * scale).T.astype(jnp.bfloat16)


def head_specs(tokens, count):
    return [pl.BlockSpec((tokens, HEAD_DIM), lambda h, pos: (0, h))] * count


def lse_spec(tokens):
    return pl.BlockSpec((1, 1, tokens), lambda h, pos: (h, 0, 0))


def forward(pos, q, ks, vs):
    tokens, width = q.shape
    heads = width // HEAD_DIM
    pairs = heads * tokens * tokens * 3
    return pl.pallas_call(
        fwd_kernel,
        grid_spec=pltpu.PrefetchScalarGridSpec(
            num_scalar_prefetch=1,
            grid=(heads,),
            in_specs=head_specs(tokens, 7),
            out_specs=head_specs(tokens, 1) + [lse_spec(tokens)],
        ),
        out_shape=[
            jax.ShapeDtypeStruct((tokens, width), jnp.bfloat16),
            jax.ShapeDtypeStruct((heads, 1, tokens), jnp.float32),
        ],
        cost_estimate=pl.CostEstimate(
            flops=pairs * HEAD_DIM * 12, bytes_accessed=tokens * width * 16, transcendentals=pairs
        ),
        name="attn_fwd",
    )(pos, q, *ks, *vs)


def backward(pos, q, ks, vs, o, lse, do):
    tokens, width = q.shape
    heads = width // HEAD_DIM
    pairs = heads * tokens * tokens * 3
    return pl.pallas_call(
        bwd_kernel,
        grid_spec=pltpu.PrefetchScalarGridSpec(
            num_scalar_prefetch=1,
            grid=(heads,),
            in_specs=head_specs(tokens, 8) + [lse_spec(tokens)] + head_specs(tokens, 1),
            out_specs=head_specs(tokens, 1)
            + [pl.BlockSpec((2, tokens, HEAD_DIM), lambda h, pos: (0, 0, h))] * 3,
        ),
        out_shape=[jax.ShapeDtypeStruct((tokens, width), jnp.bfloat16)]
        + [jax.ShapeDtypeStruct((2, tokens, width), jnp.bfloat16)] * 3,
        cost_estimate=pl.CostEstimate(
            flops=pairs * HEAD_DIM * 24, bytes_accessed=tokens * width * 32, transcendentals=pairs
        ),
        name="attn_bwd",
    )(pos, q, *ks, *vs, o, lse, do)


def shifted(block, distance):
    devices = range(lax.axis_size("seq"))
    route = [(i - distance, i) for i in devices if i - distance in devices]
    return lax.ppermute(block, "seq", route)


def ring_to(block, axis, distance):
    count = lax.axis_size(axis)
    return lax.ppermute(block, axis, [(i, (i + distance) % count) for i in range(count)])


def swapped(block):
    route = [(i, i ^ 1) for i in range(lax.axis_size("seq"))]
    return lax.ppermute(block, "seq", route)


def after(arrays, *earlier):
    return lax.optimization_barrier((*arrays, *earlier))[: len(arrays)]


def layer(queries, keys, values, out_grad, proj_weight, lengths):
    f32, bf16 = jnp.float32, jnp.bfloat16
    tokens, width = queries.shape[1:]
    place = lax.axis_index("seq")
    odd = lax.rem(place, 2) == 1
    pos = place.astype(jnp.int32).reshape(1)
    query_pos = place * tokens + jnp.arange(tokens, dtype=jnp.int32)
    live = (query_pos < lengths[0]).astype(bf16)
    grad_masked = out_grad[0] * live[:, None]

    part = width // GROUPS
    groups = [slice(g * part, (g + 1) * part) for g in range(GROUPS)]
    near = [(queries[0][:, g], keys[0][:, g], values[0][:, g]) for g in groups]
    far = []
    for _, k0, v0 in near:
        k2 = shifted(k0, 2)
        far.append((k2, shifted(v0, 2)))

    half = proj_weight.shape[1] // 2
    parity = lax.rem(place, 2)
    mine = parity * half
    w_mine = lax.all_gather(
        lax.dynamic_slice_in_dim(proj_weight, mine, half, 1), "dp", axis=0, tiled=True
    )
    w_other = swapped(w_mine)

    held, outs = [], []
    for (q, k0, v0), (k2, v2) in zip(near, far):
        if outs:
            k2, v2 = after((k2, v2), outs[-1][0])
        k1 = swapped(jnp.where(odd, k2, k0))
        v1 = swapped(jnp.where(odd, v2, v0))
        held.append((q, (k0, k1, k2), (v0, v1, v2)))
        outs.append(forward(pos, *held[-1]))

    attn = jnp.concatenate([o for o, _ in outs], 1)
    attn_pair = jnp.concatenate([attn, swapped(attn)], 0)
    chips = lax.axis_size("seq") // 2
    chip = place // 2
    own = grad_masked.shape[1] // (2 * chips)
    by_owner = grad_masked.reshape(tokens, chips, 2, own)

    def owned_by(core):
        return lax.dynamic_index_in_dim(by_owner, core, 2, False).reshape(tokens, chips * own)

    grad_pair = jnp.concatenate([owned_by(parity), swapped(owned_by(1 - parity))], 0)
    pieces = []
    for step in list(range(1, chips)) + [0]:
        at = lax.rem(chip + step, chips) * own
        piece = dot(attn_pair, lax.dynamic_slice_in_dim(grad_pair, at, own, 1), TN)
        pieces.append(piece.astype(bf16) if step else piece)
    arrived = []
    for step, piece in enumerate(pieces[:-1], 1):
        arrived.append(ring_to(piece, "seq", 2 * step))

    grad_mine = lax.dynamic_slice_in_dim(grad_masked, mine, half, 1)
    grad_other = lax.dynamic_slice_in_dim(grad_masked, half - mine, half, 1)
    (grad_mine,) = after((grad_mine,), *pieces)
    out_bwd = (dot(grad_mine, w_mine, NT) + dot(grad_other, w_other, NT)).astype(bf16)

    dqs, terms, sends = [], [], []
    for g, (q, ks, vs), (o, lse) in zip(groups, held, outs):
        do = out_bwd[:, g]
        if sends:
            (do,) = after((do,), sends[-1])
        dq, t0, t1, t2 = backward(pos, q, ks, vs, o, lse, do)
        dqs.append(dq)
        beside = swapped(t1).astype(f32)
        zero = jnp.zeros_like(beside)
        sends.append((t2.astype(f32) + jnp.where(odd, beside, zero)).astype(bf16))
        terms.append(t0.astype(f32) + jnp.where(odd, zero, beside))
    behind = []
    for send in sends:
        behind.append(shifted(send, -2))

    arrived = after(tuple(arrived), dqs[-1])
    sums = pieces[-1]
    for piece in arrived:
        sums = sums + piece.astype(f32)
    rows = proj_weight.shape[0]
    here = lax.axis_index("dp")
    count = lax.axis_size("dp")
    weight_grad = lax.dynamic_slice_in_dim(sums, here * rows, rows, 0)
    for step in range(1, count):
        at = lax.rem(here + step, count) * rows
        piece = lax.dynamic_slice_in_dim(sums, at, rows, 0).astype(bf16)
        weight_grad = weight_grad + ring_to(piece, "dp", step).astype(f32)

    totals = [(t + b.astype(f32)).astype(bf16) for t, b in zip(terms, behind)]
    return (
        jnp.concatenate(dqs, 1)[None],
        jnp.concatenate([t[0] for t in totals], 1)[None],
        jnp.concatenate([t[1] for t in totals], 1)[None],
        weight_grad,
    )


def solution(mesh):
    rows = P("dp", "seq", None)
    return jax.shard_map(
        layer,
        mesh=mesh,
        in_specs=(rows, rows, rows, rows, P("dp", None), P("dp")),
        out_specs=(rows, rows, rows, P("dp", "seq")),
        check_vma=False,
    )
```

```python
import functools

import jax
import jax.numpy as jnp
from jax import lax
from jax.experimental import pallas as pl
from jax.experimental.pallas import tpu as pltpu
from jax.sharding import PartitionSpec as P


HEAD_DIM = 128
GROUPS = 2
LOG2E = 1.4426950408889634
NEG = -1e30

NT = (((1,), (1,)), ((), ()))
NN = (((1,), (0,)), ((), ()))
TN = (((0,), (0,)), ((), ()))


def dot(a, b, dims):
    return lax.dot_general(a, b, dims, preferred_element_type=jnp.float32)


def scores_t(k, q, causal):
    s = dot(k, q, NT)
    if causal:
        key_at = lax.broadcasted_iota(jnp.int32, s.shape, 0)
        query_at = lax.broadcasted_iota(jnp.int32, s.shape, 1)
        s = jnp.where(key_at <= query_at, s, NEG)
    return s


def fwd_kernel(pos, q_ref, k0, v0, k1, k2, v1, v2, o_ref, lse_ref):
    c = HEAD_DIM ** (-0.5) * LOG2E
    q = q_ref[...]
    parts = []
    for offset, k in enumerate((k0, k1, k2)):
        parts.append(scores_t(k[...], q, offset == 0))
    tops = [jnp.max(parts[0], axis=0, keepdims=True)]
    for offset in (1, 2):
        off = jnp.where(pos[0] >= offset, 0.0, NEG)
        tops.append(jnp.max(parts[offset], axis=0, keepdims=True) + off)
    top = functools.reduce(jnp.maximum, tops) * c
    total = None
    out = None
    for offset, v in enumerate((v0, v1, v2)):
        off = jnp.where(pos[0] >= offset, 0.0, -NEG)
        e = jnp.exp2(parts[offset] * c - (top + off))
        t = jnp.sum(e, axis=0, keepdims=True)
        o = dot(v[...], e.astype(jnp.bfloat16), TN)
        total = t if total is None else total + t
        out = o if out is None else out + o
    out = out * (1.0 / total)
    o_ref[...] = out.T.astype(jnp.bfloat16)
    lse_ref[0] = top + jnp.log2(total)


def bwd_kernel(pos, q_ref, k0, v0, k1, k2, v1, v2, o_ref, lse_ref, do_ref, *rest):
    dq_ref, t0, t1, t2 = rest[-4:]
    scale = HEAD_DIM ** (-0.5)
    c = scale * LOG2E
    q = q_ref[...]
    do = do_ref[...]
    prod = do.astype(jnp.float32) * o_ref[...].astype(jnp.float32)
    delta = jnp.sum(prod.T, axis=0, keepdims=True)
    lse = lse_ref[0]
    dq = None
    for offset, (k_ref, v_ref, term) in enumerate(((k0, v0, t0), (k1, v1, t1), (k2, v2, t2))):
        k = k_ref[...]
        off = jnp.where(pos[0] >= offset, 0.0, -NEG)
        s = scores_t(k, q, offset == 0)
        p = jnp.exp2(s * c - (lse + off))
        term[1] = dot(p.astype(jnp.bfloat16), do, NN).astype(jnp.bfloat16)
        dp = dot(v_ref[...], do, NT)
        ds = (p * (dp - delta)).astype(jnp.bfloat16)
        term[0] = (dot(ds, q, NN) * scale).astype(jnp.bfloat16)
        part = dot(k, ds, TN)
        dq = part if dq is None else dq + part
    dq_ref[...] = (dq * scale).T.astype(jnp.bfloat16)


def head_specs(tokens, count):
    return [pl.BlockSpec((tokens, HEAD_DIM), lambda h, pos: (0, h))] * count


def spread_specs(tokens, count, group, per):
    def where(h, pos):
        return (0, (h // per) * (per * GROUPS) + group * per + h % per)

    return [pl.BlockSpec((tokens, HEAD_DIM), where)] * count


def lse_spec(tokens):
    return pl.BlockSpec((1, 1, tokens), lambda h, pos: (h, 0, 0))


def forward(pos, group, per, full, k1, k2, v1, v2):
    tokens, width = k1.shape
    heads = width // HEAD_DIM
    pairs = heads * tokens * tokens * 3
    return pl.pallas_call(
        fwd_kernel,
        grid_spec=pltpu.PrefetchScalarGridSpec(
            num_scalar_prefetch=1,
            grid=(heads,),
            in_specs=spread_specs(tokens, 3, group, per) + head_specs(tokens, 4),
            out_specs=head_specs(tokens, 1) + [lse_spec(tokens)],
        ),
        out_shape=[
            jax.ShapeDtypeStruct((tokens, width), jnp.bfloat16),
            jax.ShapeDtypeStruct((heads, 1, tokens), jnp.float32),
        ],
        cost_estimate=pl.CostEstimate(
            flops=pairs * HEAD_DIM * 12, bytes_accessed=tokens * width * 16, transcendentals=pairs
        ),
        name="attn_fwd",
    )(pos, *full, k1, k2, v1, v2)


def backward(pos, group, per, full, k1, k2, v1, v2, o, lse, do, held):
    tokens, width = k1.shape
    heads = width // HEAD_DIM
    pairs = heads * tokens * tokens * 3
    return pl.pallas_call(
        bwd_kernel,
        grid_spec=pltpu.PrefetchScalarGridSpec(
            num_scalar_prefetch=1,
            grid=(heads,),
            in_specs=spread_specs(tokens, 3, group, per)
            + head_specs(tokens, 5)
            + [lse_spec(tokens)]
            + head_specs(tokens, 1)
            + [pl.BlockSpec(memory_space=pl.ANY)] * len(held),
            out_specs=spread_specs(tokens, 1, group, per)
            + [pl.BlockSpec((2, tokens, HEAD_DIM), lambda h, pos: (0, 0, h))] * 3,
        ),
        out_shape=[jax.ShapeDtypeStruct((tokens, width * GROUPS), jnp.bfloat16)]
        + [jax.ShapeDtypeStruct((2, tokens, width), jnp.bfloat16)] * 3,
        cost_estimate=pl.CostEstimate(
            flops=pairs * HEAD_DIM * 24, bytes_accessed=tokens * width * 32, transcendentals=pairs
        ),
        input_output_aliases={11: 0} if held else {},
        name="attn_bwd",
    )(pos, *full, k1, k2, v1, v2, o, lse, do, *held)


def finish_kernel(pos, own_ref, beside_ref, behind_ref, *rest):
    f32 = jnp.float32
    keep = 1 - lax.rem(pos[0], 2)
    for i, out in enumerate(rest[-2:]):
        beside = jnp.where(keep == 1, beside_ref[i].astype(f32), 0.0)
        out[...] = (own_ref[i].astype(f32) + beside + behind_ref[i].astype(f32)).astype(out.dtype)


def finish(pos, group, count, own, beside, behind, held):
    _, tokens, width = own.shape
    sub = width // count
    return pl.pallas_call(
        finish_kernel,
        grid_spec=pltpu.PrefetchScalarGridSpec(
            num_scalar_prefetch=1,
            grid=(count,),
            in_specs=[pl.BlockSpec((2, tokens, sub), lambda c, pos: (0, 0, c))] * 3
            + [pl.BlockSpec(memory_space=pl.ANY)] * len(held),
            out_specs=[pl.BlockSpec((tokens, sub), lambda c, pos: (0, c * GROUPS + group))] * 2,
        ),
        out_shape=[jax.ShapeDtypeStruct((tokens, width * GROUPS), own.dtype)] * 2,
        cost_estimate=pl.CostEstimate(
            flops=6 * tokens * width, bytes_accessed=tokens * width * 16, transcendentals=0
        ),
        input_output_aliases={4: 0, 5: 1} if held else {},
        name="finish",
    )(pos, own, beside, behind, *held)


def shifted(block, distance):
    devices = range(lax.axis_size("seq"))
    route = [(i - distance, i) for i in devices if i - distance in devices]
    return lax.ppermute(block, "seq", route)


def ring_to(block, axis, distance):
    count = lax.axis_size(axis)
    return lax.ppermute(block, axis, [(i, (i + distance) % count) for i in range(count)])


def crossed(block, bit):
    return lax.ppermute(block, "seq", [(i, i ^ bit) for i in range(lax.axis_size("seq"))])


def swapped(block):
    route = [(i, i ^ 1) for i in range(lax.axis_size("seq"))]
    return lax.ppermute(block, "seq", route)


def after(arrays, *earlier):
    return lax.optimization_barrier((*arrays, *earlier))[: len(arrays)]


def layer(queries, keys, values, out_grad, proj_weight, lengths):
    f32, bf16 = jnp.float32, jnp.bfloat16
    tokens, width = queries.shape[1:]
    place = lax.axis_index("seq")
    odd = lax.rem(place, 2) == 1
    pos = place.astype(jnp.int32).reshape(1)
    query_pos = place * tokens + jnp.arange(tokens, dtype=jnp.int32)
    live = (query_pos < lengths[0]).astype(bf16)
    grad_masked = out_grad[0] * live[:, None]

    here, count = lax.axis_index("dp"), lax.axis_size("dp")
    rows = proj_weight.shape[0]
    sub = rows // GROUPS
    per = sub // HEAD_DIM
    full = (queries[0], keys[0], values[0])

    def columns(array, g):
        starts = range(g * sub, width, rows)
        return jnp.concatenate([array[:, at : at + sub] for at in starts], 1)

    near = [(columns(keys[0], g), columns(values[0], g)) for g in range(GROUPS)]
    halo = []
    for k0, v0 in near:
        k2 = shifted(k0, 2)
        halo.append((k2, shifted(v0, 2)))

    half = proj_weight.shape[1] // 2
    parity = lax.rem(place, 2)
    mine = parity * half
    weights = []
    for g in range(GROUPS):
        block = lax.dynamic_slice(proj_weight, (g * sub, mine), (sub, half))
        gathered = lax.all_gather(block, "dp", axis=0, tiled=True)
        weights.append((gathered, swapped(gathered)))
    grad_mine = lax.dynamic_slice_in_dim(grad_masked, mine, half, 1)
    grad_other = lax.dynamic_slice_in_dim(grad_masked, half - mine, half, 1)

    chips = lax.axis_size("seq") // 2
    chip = place // 2
    own = grad_masked.shape[1] // (2 * chips)

    def owned_by(core):
        return jnp.concatenate(
            [
                lax.dynamic_slice_in_dim(grad_masked, (2 * c + core) * own, own, 1)
                for c in range(chips)
            ],
            1,
        )

    grad_pair = jnp.concatenate([owned_by(parity), swapped(owned_by(1 - parity))], 0)

    dqs, terms, returned, grads = [], [], [], []
    sends = []
    for g, ((k0, v0), (k2, v2)) in enumerate(zip(near, halo)):
        if sends:
            k2, v2 = after((k2, v2), sends[-1])
        k1, v1 = jnp.where(odd, k2, k0), jnp.where(odd, v2, v0)
        side = (swapped(k1), k2, swapped(v1), v2)
        o, lse = forward(pos, g, per, full, *side)

        o_pair = jnp.concatenate([o, swapped(o)], 0)
        span = chips // 2 * own
        upper = lax.rem(chip // (chips // 2), 2)

        def product(side_of):
            return dot(o_pair, lax.dynamic_slice_in_dim(grad_pair, side_of * span, span, 1), TN)

        away = product(1 - upper).astype(bf16)
        came = crossed(away, chips)
        (last_grad,) = after((grad_mine,), away)
        kept = product(upper)

        w_mine, w_other = weights[g]
        do = (dot(last_grad, w_mine, NT) + dot(grad_other, w_other, NT)).astype(bf16)
        dq, t0, t1, t2 = backward(pos, g, per, full, *side, o, lse, do, dqs[-1:])
        dqs.append(dq)
        beside = swapped(t1)
        extra = jnp.where(odd, beside.astype(f32), 0.0)
        sends.append((t2.astype(f32) + extra).astype(bf16))
        terms.append((t0, beside))
        returned.append(shifted(sends[-1], -2))

        bit = chips // 2
        (came,) = after((came,), dq)
        kept = kept + came.astype(f32)
        while bit > 1:
            bit //= 2
            span = bit * own
            upper = lax.rem(chip // bit, 2)
            away = lax.dynamic_slice_in_dim(kept, (1 - upper) * span, span, 1).astype(bf16)
            kept = lax.dynamic_slice_in_dim(kept, upper * span, span, 1)
            came = crossed(away, 2 * bit)
            kept = kept + came.astype(f32)
        grads.append(kept)

    shares = []
    for sums in grads:
        share = lax.dynamic_slice_in_dim(sums, here * sub, sub, 0)
        for step in range(1, count):
            at = lax.rem(here + step, count) * sub
            piece = lax.dynamic_slice_in_dim(sums, at, sub, 0).astype(bf16)
            piece = ring_to(piece, "dp", step)
            share = share + piece.astype(f32)
        shares.append(share)

    totals = ()
    for g, (term, behind) in enumerate(zip(terms, returned)):
        totals = finish(pos, g, count, *term, behind, totals)
    key_grad, value_grad = totals
    return (dqs[-1][None], key_grad[None], value_grad[None], jnp.concatenate(shares, 0))


def solution(mesh):
    rows = P("dp", "seq", None)
    return jax.shard_map(
        layer,
        mesh=mesh,
        in_specs=(rows, rows, rows, rows, P("dp", None), P("dp")),
        out_specs=(rows, rows, rows, P("dp", "seq")),
        check_vma=False,
    )
```

```python
import functools

import jax
import jax.numpy as jnp
from jax import lax
from jax.experimental import pallas as pl
from jax.experimental.pallas import tpu as pltpu
from jax.sharding import PartitionSpec as P


HEAD_DIM = 128
GROUPS = 2
LOG2E = 1.4426950408889634
NEG = -1e30

NT = (((1,), (1,)), ((), ()))
NN = (((1,), (0,)), ((), ()))
TN = (((0,), (0,)), ((), ()))


def dot(a, b, dims):
    return lax.dot_general(a, b, dims, preferred_element_type=jnp.float32)


def scores_t(k, q, causal):
    s = dot(k, q, NT)
    if causal:
        key_at = lax.broadcasted_iota(jnp.int32, s.shape, 0)
        query_at = lax.broadcasted_iota(jnp.int32, s.shape, 1)
        s = jnp.where(key_at <= query_at, s, NEG)
    return s


def fwd_kernel(pos, q_ref, k0, v0, early, late, far, o_ref, lse_ref):
    c = HEAD_DIM ** (-0.5) * LOG2E
    q = q_ref[...]
    odd = lax.rem(pos[0], 2) == 1
    parts = []
    for offset in range(3):
        if offset == 1:
            k = jnp.where(odd, early[0], late[0])
        else:
            k = far[0] if offset else k0[...]
        parts.append(scores_t(k, q, offset == 0))
    tops = [jnp.max(parts[0], axis=0, keepdims=True)]
    for offset in (1, 2):
        off = jnp.where(pos[0] >= offset, 0.0, NEG)
        tops.append(jnp.max(parts[offset], axis=0, keepdims=True) + off)
    top = functools.reduce(jnp.maximum, tops) * c
    total = None
    out = None
    for offset in range(3):
        if offset == 1:
            v = jnp.where(odd, early[1], late[1])
        else:
            v = far[1] if offset else v0[...]
        off = jnp.where(pos[0] >= offset, 0.0, -NEG)
        e = jnp.exp2(parts[offset] * c - (top + off))
        t = jnp.sum(e, axis=0, keepdims=True)
        o = dot(v, e.astype(jnp.bfloat16), TN)
        total = t if total is None else total + t
        out = o if out is None else out + o
    out = out * (1.0 / total)
    o_ref[...] = out.T.astype(jnp.bfloat16)
    lse_ref[0] = top + jnp.log2(total)


def bwd_kernel(pos, q_ref, k0, v0, early, late, far, o_ref, lse_ref, do_ref, *rest):
    dq_ref, t0, t1, t2 = rest[-4:]
    scale = HEAD_DIM ** (-0.5)
    c = scale * LOG2E
    q = q_ref[...]
    do = do_ref[...]
    odd = lax.rem(pos[0], 2) == 1
    prod = do.astype(jnp.float32) * o_ref[...].astype(jnp.float32)
    delta = jnp.sum(prod.T, axis=0, keepdims=True)
    lse = lse_ref[0]
    dq = None
    for offset, term in enumerate((t0, t1, t2)):
        if offset == 1:
            k, v = jnp.where(odd, early[0], late[0]), jnp.where(odd, early[1], late[1])
        else:
            k, v = (far[0], far[1]) if offset else (k0[...], v0[...])
        off = jnp.where(pos[0] >= offset, 0.0, -NEG)
        s = scores_t(k, q, offset == 0)
        p = jnp.exp2(s * c - (lse + off))
        term[1] = dot(p.astype(jnp.bfloat16), do, NN).astype(jnp.bfloat16)
        dp = dot(v, do, NT)
        ds = (p * (dp - delta)).astype(jnp.bfloat16)
        term[0] = (dot(ds, q, NN) * scale).astype(jnp.bfloat16)
        part = dot(k, ds, TN)
        dq = part if dq is None else dq + part
    dq_ref[...] = (dq * scale).T.astype(jnp.bfloat16)


def pair_specs(tokens, count):
    return [pl.BlockSpec((2, tokens, HEAD_DIM), lambda h, pos: (0, 0, h))] * count


def head_specs(tokens, count):
    return [pl.BlockSpec((tokens, HEAD_DIM), lambda h, pos: (0, h))] * count


def spread_specs(tokens, count, group, per):
    def where(h, pos):
        return (0, (h // per) * (per * GROUPS) + group * per + h % per)

    return [pl.BlockSpec((tokens, HEAD_DIM), where)] * count


def lse_spec(tokens):
    return pl.BlockSpec((1, 1, tokens), lambda h, pos: (h, 0, 0))


def forward(pos, group, per, full, early, late, far):
    _, tokens, width = far.shape
    heads = width // HEAD_DIM
    pairs = heads * tokens * tokens * 3
    return pl.pallas_call(
        fwd_kernel,
        grid_spec=pltpu.PrefetchScalarGridSpec(
            num_scalar_prefetch=1,
            grid=(heads,),
            in_specs=spread_specs(tokens, 3, group, per) + pair_specs(tokens, 3),
            out_specs=head_specs(tokens, 1) + [lse_spec(tokens)],
        ),
        out_shape=[
            jax.ShapeDtypeStruct((tokens, width), jnp.bfloat16),
            jax.ShapeDtypeStruct((heads, 1, tokens), jnp.float32),
        ],
        cost_estimate=pl.CostEstimate(
            flops=pairs * HEAD_DIM * 12, bytes_accessed=tokens * width * 16, transcendentals=pairs
        ),
        name="attn_fwd",
    )(pos, *full, early, late, far)


def backward(pos, group, per, full, early, late, far, o, lse, do, held):
    _, tokens, width = far.shape
    heads = width // HEAD_DIM
    pairs = heads * tokens * tokens * 3
    return pl.pallas_call(
        bwd_kernel,
        grid_spec=pltpu.PrefetchScalarGridSpec(
            num_scalar_prefetch=1,
            grid=(heads,),
            in_specs=spread_specs(tokens, 3, group, per)
            + pair_specs(tokens, 3)
            + head_specs(tokens, 1)
            + [lse_spec(tokens)]
            + head_specs(tokens, 1)
            + [pl.BlockSpec(memory_space=pl.ANY)] * len(held),
            out_specs=spread_specs(tokens, 1, group, per)
            + pair_specs(tokens, 3),
        ),
        out_shape=[jax.ShapeDtypeStruct((tokens, width * GROUPS), jnp.bfloat16)]
        + [jax.ShapeDtypeStruct((2, tokens, width), jnp.bfloat16)] * 3,
        cost_estimate=pl.CostEstimate(
            flops=pairs * HEAD_DIM * 24, bytes_accessed=tokens * width * 32, transcendentals=pairs
        ),
        input_output_aliases={10: 0} if held else {},
        name="attn_bwd",
    )(pos, *full, early, late, far, o, lse, do, *held)


def finish_kernel(pos, own_ref, beside_ref, behind_ref, *rest):
    f32 = jnp.float32
    keep = 1 - lax.rem(pos[0], 2)
    for i, out in enumerate(rest[-2:]):
        beside = jnp.where(keep == 1, beside_ref[i].astype(f32), 0.0)
        out[...] = (own_ref[i].astype(f32) + beside + behind_ref[i].astype(f32)).astype(out.dtype)


def finish(pos, group, count, own, beside, behind, held):
    _, tokens, width = own.shape
    sub = width // count
    return pl.pallas_call(
        finish_kernel,
        grid_spec=pltpu.PrefetchScalarGridSpec(
            num_scalar_prefetch=1,
            grid=(count,),
            in_specs=[pl.BlockSpec((2, tokens, sub), lambda c, pos: (0, 0, c))] * 3
            + [pl.BlockSpec(memory_space=pl.ANY)] * len(held),
            out_specs=[pl.BlockSpec((tokens, sub), lambda c, pos: (0, c * GROUPS + group))] * 2,
        ),
        out_shape=[jax.ShapeDtypeStruct((tokens, width * GROUPS), own.dtype)] * 2,
        cost_estimate=pl.CostEstimate(
            flops=6 * tokens * width, bytes_accessed=tokens * width * 16, transcendentals=0
        ),
        input_output_aliases={4: 0, 5: 1} if held else {},
        name="finish",
    )(pos, own, beside, behind, *held)


def shifted(block, distance):
    devices = range(lax.axis_size("seq"))
    route = [(i - distance, i) for i in devices if i - distance in devices]
    return lax.ppermute(block, "seq", route)


def ring_to(block, axis, distance):
    count = lax.axis_size(axis)
    return lax.ppermute(block, axis, [(i, (i + distance) % count) for i in range(count)])


def crossed(block, bit):
    return lax.ppermute(block, "seq", [(i, i ^ bit) for i in range(lax.axis_size("seq"))])


def swapped(block):
    route = [(i, i ^ 1) for i in range(lax.axis_size("seq"))]
    return lax.ppermute(block, "seq", route)


def after(arrays, *earlier):
    return lax.optimization_barrier((*arrays, *earlier))[: len(arrays)]


def layer(queries, keys, values, out_grad, proj_weight, lengths):
    f32, bf16 = jnp.float32, jnp.bfloat16
    tokens, width = queries.shape[1:]
    place = lax.axis_index("seq")
    odd = lax.rem(place, 2) == 1
    pos = place.astype(jnp.int32).reshape(1)
    query_pos = place * tokens + jnp.arange(tokens, dtype=jnp.int32)
    live = (query_pos < lengths[0]).astype(bf16)
    grad_masked = out_grad[0] * live[:, None]

    here, count = lax.axis_index("dp"), lax.axis_size("dp")
    rows = proj_weight.shape[0]
    sub = rows // GROUPS
    per = sub // HEAD_DIM
    full = (queries[0], keys[0], values[0])

    def columns(array, g):
        starts = range(g * sub, width, rows)
        return jnp.concatenate([array[:, at : at + sub] for at in starts], 1)

    evens = range(0, lax.axis_size("seq"), 2)
    near = [jnp.stack([columns(keys[0], g), columns(values[0], g)]) for g in range(GROUPS)]
    halo = []
    for block in near:
        halo.append(shifted(block, 2))
    sooner = []
    for block in near:
        sooner.append(lax.ppermute(block, "seq", [(i, i + 1) for i in evens]))

    half = proj_weight.shape[1] // 2
    parity = lax.rem(place, 2)
    mine = parity * half
    weights = []
    for g in range(GROUPS):
        block = lax.dynamic_slice(proj_weight, (g * sub, mine), (sub, half))
        gathered = lax.all_gather(block, "dp", axis=0, tiled=True)
        weights.append((gathered, swapped(gathered)))
    grad_mine = lax.dynamic_slice_in_dim(grad_masked, mine, half, 1)
    grad_other = lax.dynamic_slice_in_dim(grad_masked, half - mine, half, 1)

    chips = lax.axis_size("seq") // 2
    chip = place // 2
    own = grad_masked.shape[1] // (2 * chips)

    def owned_by(core):
        return jnp.concatenate(
            [
                lax.dynamic_slice_in_dim(grad_masked, (2 * c + core) * own, own, 1)
                for c in range(chips)
            ],
            1,
        )

    grad_pair = jnp.concatenate([owned_by(parity), swapped(owned_by(1 - parity))], 0)

    dqs, terms, returned, grads = [], [], [], []
    sends = []
    for g in range(GROUPS):
        later = lax.ppermute(halo[g], "seq", [(i + 1, i) for i in evens])
        if sends:
            (later,) = after((later,), sends[-1])
        side = (sooner[g], later, halo[g])
        o, lse = forward(pos, g, per, full, *side)

        o_pair = jnp.concatenate([o, swapped(o)], 0)
        span = chips // 2 * own
        upper = lax.rem(chip // (chips // 2), 2)

        def product(side_of):
            return dot(o_pair, lax.dynamic_slice_in_dim(grad_pair, side_of * span, span, 1), TN)

        away = product(1 - upper).astype(bf16)
        came = crossed(away, chips)
        (last_grad,) = after((grad_mine,), away)
        kept = product(upper)

        w_mine, w_other = weights[g]
        do = (dot(last_grad, w_mine, NT) + dot(grad_other, w_other, NT)).astype(bf16)
        dq, t0, t1, t2 = backward(pos, g, per, full, *side, o, lse, do, dqs[-1:])
        dqs.append(dq)
        beside = swapped(t1)
        extra = jnp.where(odd, beside.astype(f32), 0.0)
        sends.append((t2.astype(f32) + extra).astype(bf16))
        terms.append((t0, beside))
        returned.append(shifted(sends[-1], -2))

        bit = chips // 2
        (came,) = after((came,), dq)
        kept = kept + came.astype(f32)
        while bit > 1:
            bit //= 2
            span = bit * own
            upper = lax.rem(chip // bit, 2)
            away = lax.dynamic_slice_in_dim(kept, (1 - upper) * span, span, 1).astype(bf16)
            kept = lax.dynamic_slice_in_dim(kept, upper * span, span, 1)
            came = crossed(away, 2 * bit)
            kept = kept + came.astype(f32)
        grads.append(kept)

    shares = []
    for sums in grads:
        share = lax.dynamic_slice_in_dim(sums, here * sub, sub, 0)
        for step in range(1, count):
            at = lax.rem(here + step, count) * sub
            piece = lax.dynamic_slice_in_dim(sums, at, sub, 0).astype(bf16)
            piece = ring_to(piece, "dp", step)
            share = share + piece.astype(f32)
        shares.append(share)

    totals = ()
    for g, (term, behind) in enumerate(zip(terms, returned)):
        totals = finish(pos, g, count, *term, behind, totals)
    key_grad, value_grad = totals
    return (dqs[-1][None], key_grad[None], value_grad[None], jnp.concatenate(shares, 0))


def solution(mesh):
    rows = P("dp", "seq", None)
    return jax.shard_map(
        layer,
        mesh=mesh,
        in_specs=(rows, rows, rows, rows, P("dp", None), P("dp")),
        out_specs=(rows, rows, rows, P("dp", "seq")),
        check_vma=False,
    )
```
